8 devices in a mesh: dp: 1 (over z), sp: 2 (over y), cp: 4 (over x, core).
Axes of the slice: x: 2, y: 2, z: 1, core: 2. Of those that a mesh axis runs over, the one named last changes fastest.
Arguments:
- hidden: bfloat16 [8, 2048, 1920], P('dp', ('cp', 'sp'))
- seg_ids: int32 [8, 2048], P('dp', ('cp', 'sp'))
- w_qkv: bfloat16 [1920, 3, 30, 64], replicated
- w_out: bfloat16 [30, 64, 1920], replicated
Outputs:
- output: bfloat16 [8, 2048, 1920], P('dp', ('cp', 'sp'))
All inputs are finite; a program needn't handle non-finite values.
Results may differ from the reference program's by a relative error of at most 0.00536751.
Values are sent between devices in bfloat16 or wider.
A program may use at most 1 GiB of HBM per device.

```python
import jax
import jax.numpy as jnp
from jax import lax

BATCH = 8
SEQ = 2048
DIM = 1920
HEADS = 30
HEAD = 64
QUERY_BLOCK = 256
CUTS = 3


def draw_segments(seg_key):
    key_first, key_rest = jax.random.split(seg_key)
    first_cut = jax.random.randint(key_first, (BATCH, 1), SEQ // 2 + SEQ // 8, SEQ - SEQ // 8)
    offsets = jax.random.randint(key_rest, (BATCH, CUTS - 1), 0, 1 << 20) % (SEQ - first_cut)
    cut_points = jnp.concatenate([first_cut, first_cut + offsets], axis=1)
    positions = jnp.arange(SEQ, dtype=jnp.int32)
    return jnp.sum(positions[None, :, None] >= cut_points[:, None, :], axis=-1).astype(jnp.int32)


def setup_inputs(seed: int = 0, part: int = 0) -> dict:
    part_key = jax.random.fold_in(jax.random.key(seed), part)
    key_hidden, key_seg = jax.random.split(part_key)
    key_qkv, key_out = jax.random.split(jax.random.key(seed + 1))
    hidden = jax.random.normal(key_hidden, (BATCH, SEQ, DIM), jnp.float32)
    qkv_gain = jnp.where(jnp.arange(3) < 2, (2.0 / DIM) ** 0.5, DIM ** -0.5)
    w_qkv = jax.random.normal(key_qkv, (DIM, 3, HEADS, HEAD), jnp.float32) * qkv_gain[:, None, None]
    out_gain = (HEADS * HEAD) ** -0.5 * SEQ ** 0.5 / 10.0
    w_out = jax.random.normal(key_out, (HEADS, HEAD, DIM), jnp.float32) * out_gain
    return {'hidden': hidden.astype(jnp.bfloat16), 'seg_ids': draw_segments(key_seg), 'w_qkv': w_qkv.astype(jnp.bfloat16), 'w_out': w_out.astype(jnp.bfloat16)}


def reference(hidden, seg_ids, w_qkv, w_out):
    projected = jnp.dot(hidden.reshape(BATCH * SEQ, DIM), w_qkv.reshape(DIM, 3 * HEADS * HEAD), preferred_element_type=jnp.float32)
    projected = projected.astype(jnp.bfloat16).reshape(BATCH, SEQ, 3, HEADS, HEAD)
    per_head = jnp.transpose(projected, (3, 2, 0, 1, 4))
    num_blocks = SEQ // QUERY_BLOCK
    seg_blocks = jnp.transpose(seg_ids.reshape(BATCH, num_blocks, QUERY_BLOCK), (1, 0, 2))
    logit_scale = HEAD ** -0.5

    def one_head(head_qkv):
        keys_f32 = head_qkv[1].astype(jnp.float32)
        values_f32 = head_qkv[2].astype(jnp.float32)
        query_blocks = jnp.transpose(head_qkv[0].reshape(BATCH, num_blocks, QUERY_BLOCK, HEAD), (1, 0, 2, 3))

        def one_block(block_args):
            query_blk, seg_blk = block_args
            scores = jnp.einsum('bqd,bkd->bqk', query_blk.astype(jnp.float32), keys_f32) * logit_scale
            allowed = seg_blk[:, :, None] == seg_ids[:, None, :]
            scores = jnp.where(allowed, scores, -jnp.inf)
            row_max = jnp.max(scores, axis=-1, keepdims=True)
            weights = jnp.exp(scores - row_max)
            row_sum = jnp.sum(weights, axis=-1, keepdims=True)
            mixed_vals = jnp.einsum('bqk,bkd->bqd', weights.astype(jnp.bfloat16).astype(jnp.float32), values_f32)
            return (mixed_vals / row_sum).astype(jnp.bfloat16)

        out_blocks = lax.map(one_block, (query_blocks, seg_blocks))
        return jnp.transpose(out_blocks, (1, 0, 2, 3)).reshape(BATCH, SEQ, HEAD)

    attn_heads = lax.map(one_head, per_head)
    attn_flat = jnp.transpose(attn_heads, (1, 2, 0, 3)).reshape(BATCH * SEQ, HEADS * HEAD)
    result = jnp.dot(attn_flat, w_out.reshape(HEADS * HEAD, DIM), preferred_element_type=jnp.float32)
    return result.astype(jnp.bfloat16).reshape(BATCH, SEQ, DIM)
```

```python
import functools
import math

import jax
import jax.numpy as jnp
from jax import lax
from jax.experimental import pallas as pl
from jax.experimental.pallas import tpu as pltpu
from jax.sharding import PartitionSpec as P


BLK = 256
LANES = 128
MASKED = -0.7 * 3.4028235e38


def attention_kernel(order_ref, counts_ref, qa_ref, qb_ref, k0_ref, k1_ref, k2_ref, k3_ref, qid_ref, kid_ref, oa_ref, ob_ref, kv_ref, *, scale):
    head = pl.program_id(0)
    even = lax.rem(head, 2) == 0
    half = k0_ref.shape[0]
    for n, ref in enumerate((k0_ref, k1_ref, k2_ref, k3_ref)):
        kv_ref[n * half:(n + 1) * half, :] = ref[...]
    lane = lax.broadcasted_iota(jnp.int32, (BLK, LANES), 1)
    left = lane < LANES // 2
    out_lanes = left == even

    def load_kv(slot):
        start = pl.multiple_of(slot * BLK, BLK)
        return kv_ref[pl.ds(start, BLK), :]

    def absorb(q, kvs, masks, carry):
        m, l, acc = carry
        ss = [lax.dot_general(q, kv, (((1,), (1,)), ((), ())), preferred_element_type=jnp.float32) for kv in kvs]
        if masks is not None:
            ss = [jnp.where(mask, s, MASKED) for s, mask in zip(ss, masks)]
        mx = ss[0]
        for s in ss[1:]:
            mx = jnp.maximum(mx, s)
        m_new = jnp.maximum(m, jnp.max(mx, axis=1, keepdims=True))
        alpha = jnp.exp2((m - m_new) * scale)
        l = l * alpha
        acc = acc * alpha
        for s, kv in zip(ss, kvs):
            p = jnp.exp2((s - m_new) * scale)
            for j in range(BLK // LANES):
                l = l + p[:, j * LANES:(j + 1) * LANES]
            acc = acc + jnp.dot(p.astype(jnp.bfloat16), kv, preferred_element_type=jnp.float32)
        return m_new, l, acc

    per_ref = half // BLK
    for qn in range(2 * per_ref):
        q_ref, o_ref = ((qa_ref, oa_ref), (qb_ref, ob_ref))[qn // per_ref]
        rows = slice((qn % per_ref) * BLK, (qn % per_ref + 1) * BLK)
        tile = q_ref[rows, :]
        q = jnp.where(left != even, tile, jnp.zeros_like(tile))
        pairs = counts_ref[qn, 0] // 2
        active = counts_ref[qn, 1]

        def full_step(t, carry, qn=qn, q=q):
            return absorb(q, [load_kv(order_ref[qn, 2 * t]), load_kv(order_ref[qn, 2 * t + 1])], None, carry)

        def masked_step(t, carry, qn=qn, q=q):
            slot = order_ref[qn, t]
            qid = qid_ref[qn * BLK:(qn + 1) * BLK, :]
            kid = kid_ref[pl.ds(slot, 1), :]
            mask = jnp.concatenate([qid] * (BLK // LANES), axis=1) == kid
            return absorb(q, [load_kv(slot)], [mask], carry)

        carry = (jnp.full((BLK, 1), MASKED, jnp.float32), jnp.zeros((BLK, LANES), jnp.float32), jnp.zeros((BLK, LANES), jnp.float32))
        carry = lax.fori_loop(0, pairs, full_step, carry)
        carry = lax.fori_loop(2 * pairs, active, masked_step, carry)
        _, l, acc = carry
        out = (acc / jnp.sum(l, axis=1, keepdims=True)).astype(jnp.bfloat16)

        @pl.when(even)
        def _(out=out, o_ref=o_ref, rows=rows):
            o_ref[rows, :] = jnp.where(left, out, jnp.zeros_like(out))

        @pl.when(jnp.logical_not(even))
        def _(out=out, o_ref=o_ref, rows=rows):
            o_ref[rows, :] = jnp.where(left, o_ref[rows, :], out)


def attention(order, counts, qa, qb, kvs, qid, kid, heads, head_dim):
    half = qa.shape[0]
    width = qa.shape[1]
    scale = math.log2(math.e) * head_dim ** -0.5
    kv_spec = pl.BlockSpec((half, LANES), lambda h, *_: (0, h))
    pair_spec = pl.BlockSpec((half, LANES), lambda h, *_: (0, h // 2))
    whole = lambda a: pl.BlockSpec(a.shape, lambda h, *_: (0, 0))
    out = jax.ShapeDtypeStruct((half, width), jnp.bfloat16)
    scores = 2 * half * 4 * half * heads
    return pl.pallas_call(
        functools.partial(attention_kernel, scale=scale),
        out_shape=(out, out),
        grid_spec=pltpu.PrefetchScalarGridSpec(
            num_scalar_prefetch=2,
            grid=(heads,),
            in_specs=[pair_spec, pair_spec] + [kv_spec] * 4 + [whole(qid), whole(kid)],
            out_specs=(pair_spec, pair_spec),
            scratch_shapes=[pltpu.VMEM((4 * half, LANES), jnp.bfloat16)],
        ),
        compiler_params=pltpu.CompilerParams(dimension_semantics=("arbitrary",)),
        cost_estimate=pl.CostEstimate(flops=scores * 2 * LANES * 2, bytes_accessed=(4 * half * heads * LANES + 4 * half * width) * 2, transcendentals=scores),
    )(order, counts, qa, qb, *kvs, qid, kid)


def solution(mesh):
    token_spec = P('dp', ('cp', 'sp'), None)
    seg_spec = P('dp', ('cp', 'sp'))
    axes = ('sp', 'cp')
    num = mesh.shape['cp'] * mesh.shape['sp']

    def core_of(f):
        return (f >> 1) & 1

    def stage1(f):
        return f ^ 1 if core_of(f) == 0 else f ^ 4

    def stage2(f):
        return f ^ 4 if core_of(f) == 0 else f ^ 1

    def spot(f):
        return (f & 1) * mesh.shape['cp'] + (f >> 1)

    perm_core = [(spot(f), spot(f ^ 2)) for f in range(num)]
    perm_one = [(spot(f), spot(stage1(f))) for f in range(num)]
    perm_two = [(spot(f), spot(stage2(f))) for f in range(num)]
    block_table = []
    for f in range(num):
        g = stage2(f)
        block_table.append([spot(b) for b in (f, f ^ 2, stage1(f), stage1(f) ^ 2, g, g ^ 2, stage1(g), stage1(g) ^ 2)])

    def local_layer(hidden, seg_ids, w_qkv, w_out):
        batch, tokens, dim = hidden.shape
        heads, head_dim = w_out.shape[0], w_out.shape[1]
        mine = heads // 2
        padded = mine + mine % 2
        per_core = batch // 2
        me = lax.axis_index('cp') * mesh.shape['sp'] + lax.axis_index('sp')
        core = (me // 2) % 2
        hsel = jnp.where(core == 0, me % 2, me // 4)
        nblk = len(block_table[0])

        def permute(x, perm):
            return lax.ppermute(x, axes, perm)

        keep = lax.dynamic_slice_in_dim(hidden, core * per_core, per_core, 0)
        give = lax.dynamic_slice_in_dim(hidden, (1 - core) * per_core, per_core, 0)
        x_chip, x_next = [], []
        for i in range(per_core):
            got = permute(give[i], perm_core)
            x_chip.append(jnp.concatenate([keep[i], got], axis=0))
            x_next.append(permute(x_chip[i], perm_one))

        wt = lax.dynamic_slice_in_dim(jnp.transpose(w_qkv, (1, 2, 3, 0)), hsel * mine, mine, 1)
        odd = (jnp.arange(mine) % 2 == 1)[:, None, None]
        w_kv = jnp.stack([jnp.where(odd, wt[1], wt[2]), jnp.where(odd, wt[2], wt[1])], axis=1).reshape(mine * 2 * head_dim, dim)
        w_q = jnp.pad(wt[0], ((0, padded - mine), (0, 0), (0, 0))).reshape(padded // 2, 2, head_dim, dim)
        w_q = jnp.flip(w_q, axis=1).reshape(padded * head_dim, dim)

        def out_weight(first):
            part = lax.dynamic_slice_in_dim(w_out, first * mine, mine, 0)
            return jnp.pad(part, ((0, padded - mine), (0, 0), (0, 0))).reshape(padded * head_dim, dim)

        wo_mine, wo_other = out_weight(hsel), out_weight(1 - hsel)

        seg_all = lax.all_gather(seg_ids, axes, axis=0)
        blocks = jnp.asarray(block_table, jnp.int32)[me]
        seg_mine = lax.dynamic_slice_in_dim(seg_all, core * per_core, per_core, 1)
        seg_mine = jnp.transpose(jnp.take(seg_mine, blocks, axis=0), (1, 0, 2))
        first, last = seg_mine[:, :, 0], seg_mine[:, :, -1]
        nq = nblk // 2
        qf, ql = first[:, :nq, None], last[:, :nq, None]
        kf, kl = first[:, None, :], last[:, None, :]
        meets = (kf <= ql) & (qf <= kl)
        full = meets & (qf == ql) & (kf == kl)
        part = meets & ~full
        n_full = jnp.sum(full, axis=-1, dtype=jnp.int32)
        n_meet = jnp.sum(meets, axis=-1, dtype=jnp.int32)
        before = (jnp.arange(nblk)[:, None] < jnp.arange(nblk)[None, :]).astype(jnp.int32)
        rank_full = jnp.sum(full.astype(jnp.int32)[..., :, None] * before, axis=-2)
        rank_part = jnp.sum(part.astype(jnp.int32)[..., :, None] * before, axis=-2) + n_full[..., None]
        place = jnp.where(full, rank_full, jnp.where(part, rank_part, nblk))
        order = jnp.sum((place[..., :, None] == jnp.arange(nblk)) * jnp.arange(nblk, dtype=jnp.int32)[:, None], axis=-2).astype(jnp.int32)
        counts = jnp.stack([n_full, n_meet], axis=-1)

        def project(x, w):
            return lax.dot_general(x, w, (((1,), (1,)), ((), ())), preferred_element_type=jnp.float32).astype(jnp.bfloat16)

        kv_chip = [project(x, w_kv) for x in x_chip]
        kv_far = [[permute(kv, perm_two)] for kv in kv_chip]
        kv_next = [project(x, w_kv) for x in x_next]
        for i in range(per_core):
            kv_far[i].append(permute(kv_next[i], perm_two))
        q_chip = [project(x, w_q) for x in x_chip]
        q_next = [project(x, w_q) for x in x_next]

        result = jnp.zeros((batch, tokens, dim), jnp.bfloat16)
        for i in range(per_core):
            seg_i = seg_mine[i]
            qid = jnp.broadcast_to(seg_i[:nq].reshape(nq * tokens, 1), (nq * tokens, LANES))
            o_chip, o_next = attention(order[i], counts[i], q_chip[i], q_next[i], [kv_chip[i], kv_next[i]] + kv_far[i], qid, seg_i, mine, head_dim)
            o_got = permute(o_next, perm_one)
            y = jnp.dot(o_chip, wo_mine, preferred_element_type=jnp.float32)
            y = (y + jnp.dot(o_got, wo_other, preferred_element_type=jnp.float32)).astype(jnp.bfloat16)
            y_got = permute(y[tokens:], perm_core)
            result = lax.dynamic_update_slice(result, y[None, :tokens], (core * per_core + i, 0, 0))
            result = lax.dynamic_update_slice(result, y_got[None], ((1 - core) * per_core + i, 0, 0))
        return result

    return jax.shard_map(local_layer, mesh=mesh, in_specs=(token_spec, seg_spec, P(), P()), out_specs=token_spec, check_vma=False)
```

```python
import functools
import math

import jax
import jax.numpy as jnp
from jax import lax
from jax.experimental import pallas as pl
from jax.experimental.pallas import tpu as pltpu
from jax.sharding import PartitionSpec as P


BLK = 256
LANES = 128
GROUP = 4
MASKED = -0.7 * 3.4028235e38
NT = (((1,), (1,)), ((), ()))


def project_kernel(sel_ref, x0, x1, x2, x3, w_ref, q_ref, kv_ref, x_scr, w_scr, x_sem, w_sem, *, heads, head_dim):
    g = pl.program_id(0)
    xs = (x0, x1, x2, x3)
    groups = [list(range(s, min(s + GROUP, heads))) for s in range(0, heads, GROUP)]
    kv_row = GROUP * head_dim

    def x_copies():
        return [pltpu.make_async_copy(x, x_scr.at[pl.ds(n * BLK, BLK), :], x_sem.at[n]) for n, x in enumerate(xs)]

    def w_copies(n):
        first = sel_ref[0]
        out = []
        for k, h in enumerate(groups[n]):
            swap = k % 2
            rows = [k + 1 - 2 * swap, kv_row // head_dim + 2 * k + 1 - swap, kv_row // head_dim + 2 * k + swap]
            for j, row in enumerate(rows):
                out.append(pltpu.make_async_copy(w_ref.at[j, first + h], w_scr.at[n, pl.ds(row * head_dim, head_dim), :], w_sem.at[n, 3 * k + j]))
        return out

    @pl.when(g == 0)
    def _():
        for c in x_copies():
            c.start()
        for n in range(len(groups)):
            for c in w_copies(n):
                c.start()
        for n, group in enumerate(groups):
            for k in range(len(group), GROUP):
                swap = k % 2
                zero = jnp.zeros((head_dim, w_scr.shape[2]), w_scr.dtype)
                w_scr[n, (k + 1 - 2 * swap) * head_dim:(k + 2 - 2 * swap) * head_dim, :] = zero
                for r in range(2):
                    row = kv_row + (2 * k + r) * head_dim
                    w_scr[n, row:row + head_dim, :] = zero
        for c in x_copies():
            c.wait()

    for n in range(len(groups)):
        @pl.when(g == n)
        def _(n=n):
            for c in w_copies(n):
                c.wait()

    half = x_scr.shape[0] // 2
    for r in range(2):
        x = x_scr[r * half:(r + 1) * half, :]
        for n in range(w_scr.shape[1] // BLK):
            w = w_scr[g, n * BLK:(n + 1) * BLK, :]
            out = lax.dot_general(x, w, NT, preferred_element_type=jnp.float32).astype(jnp.bfloat16)
            if n == 0:
                q_ref[r * half:(r + 1) * half, :] = out
            else:
                kv_ref[r * half:(r + 1) * half, (n - 1) * BLK:n * BLK] = out


def project_all(sel, xs, wt, heads, head_dim):
    rows, dim = 4 * xs[0].shape[0], xs[0].shape[1]
    steps = pl.cdiv(heads, GROUP)
    wide = GROUP * head_dim
    out = (jax.ShapeDtypeStruct((rows, steps * wide), jnp.bfloat16), jax.ShapeDtypeStruct((rows, heads * 2 * head_dim), jnp.bfloat16))
    hbm = pl.BlockSpec(memory_space=pl.ANY)
    return pl.pallas_call(
        functools.partial(project_kernel, heads=heads, head_dim=head_dim),
        out_shape=out,
        grid_spec=pltpu.PrefetchScalarGridSpec(
            num_scalar_prefetch=1,
            grid=(steps,),
            in_specs=[hbm] * 5,
            out_specs=(pl.BlockSpec((rows, wide), lambda g, *_: (0, g)), pl.BlockSpec((rows, 2 * wide), lambda g, *_: (0, g))),
            scratch_shapes=[
                pltpu.VMEM((rows, dim), jnp.bfloat16),
                pltpu.VMEM((steps, 3 * wide, dim), jnp.bfloat16),
                pltpu.SemaphoreType.DMA((4,)),
                pltpu.SemaphoreType.DMA((steps, 3 * GROUP)),
            ],
        ),
        compiler_params=pltpu.CompilerParams(dimension_semantics=("arbitrary",)),
        cost_estimate=pl.CostEstimate(flops=2 * rows * dim * 3 * heads * head_dim, bytes_accessed=2 * (rows * dim * 3 + 3 * heads * head_dim * dim), transcendentals=0),
    )(sel, *xs, wt)


def attention_kernel(cut_ref, q_ref, own_ref, far_ref, oa_ref, ob_ref, kv_scr, m_scr, l_scr, acc_scr, list_ref, sem, *, scale, heads):
    i = pl.program_id(0)
    rows = own_ref.shape[0]
    blocks = 2 * rows // BLK
    ncut = cut_ref.shape[1]
    groups = [list(range(s, min(s + GROUP, heads))) for s in range(0, heads, GROUP)]
    left = lax.broadcasted_iota(jnp.int32, (BLK, LANES), 1) < LANES // 2

    def copies(n):
        cols = pl.ds(groups[n][0] * LANES, len(groups[n]) * LANES)
        return [pltpu.make_async_copy(ref.at[:, cols], kv_scr.at[pl.ds(r * rows, rows), cols], sem.at[n, r]) for r, ref in enumerate((own_ref, far_ref))]

    @pl.when(i == 0)
    def _():
        for n in range(len(groups)):
            for c in copies(n):
                c.start()

    def id_at(block, pos):
        return sum((cut_ref[block, d] <= pos).astype(jnp.int32) for d in range(ncut))

    qf, ql = id_at(i, 0), id_at(i, BLK - 1)
    count = jnp.int32(0)
    kinds = []
    for b in range(blocks):
        kf, kl = id_at(b, 0), id_at(b, BLK - 1)
        meets = ((kf <= ql) & (qf <= kl)).astype(jnp.int32)
        full = meets * ((qf == ql) & (kf == kl)).astype(jnp.int32)
        kinds.append(meets - full)
        list_ref[count] = b
        count = count + full
    pairs = count // 2
    for b in range(blocks):
        list_ref[count] = b
        count = count + kinds[b]

    def absorb(group, qs, slots, mask):
        starts = [pl.multiple_of(slot * BLK, BLK) for slot in slots]

        def kv_of(h):
            tiles = [kv_scr[pl.ds(s, BLK), h * LANES:(h + 1) * LANES] for s in starts]
            return tiles[0] if len(tiles) == 1 else jnp.concatenate(tiles, axis=0)

        def scores(k):
            s = lax.dot_general(qs[k], kv_of(group[k]), NT, preferred_element_type=jnp.float32)
            return s if mask is None else jnp.where(mask, s, MASKED)

        ahead = scores(0)
        for k, h in enumerate(group):
            s = ahead
            if k + 1 < len(group):
                ahead = scores(k + 1)
            parts = [s[:, j * LANES:(j + 1) * LANES] for j in range(len(slots) * BLK // LANES)]
            mx = functools.reduce(jnp.maximum, parts)
            m_old = m_scr[k]
            m_new = jnp.maximum(m_old, jnp.max(mx, axis=1, keepdims=True))
            alpha = jnp.exp2((m_old - m_new) * scale)
            ps = [jnp.exp2((part - m_new) * scale) for part in parts]
            m_scr[k] = m_new
            l_scr[k] = l_scr[k] * alpha + functools.reduce(jnp.add, ps)
            p = jnp.concatenate([p.astype(jnp.bfloat16) for p in ps], axis=1)
            acc_scr[k] = acc_scr[k] * alpha + jnp.dot(p, kv_of(h), preferred_element_type=jnp.float32)

    for n, group in enumerate(groups):
        @pl.when(i == 0)
        def _(n=n):
            for c in copies(n):
                c.wait()

        qs = []
        for h in group:
            tile = q_ref[:, (h // 2) * LANES:(h // 2 + 1) * LANES]
            zero = jnp.zeros_like(tile)
            qs.append(jnp.where(left, tile, zero) if h % 2 else jnp.where(left, zero, tile))
        for k in range(len(group)):
            m_scr[k] = jnp.full((BLK, LANES), MASKED, jnp.float32)
            l_scr[k] = jnp.zeros((BLK, LANES), jnp.float32)
            acc_scr[k] = jnp.zeros((BLK, LANES), jnp.float32)

        @pl.loop(0, pairs)
        def _(t, group=group, qs=qs):
            absorb(group, qs, [list_ref[2 * t], list_ref[2 * t + 1]], None)

        @pl.loop(2 * pairs, count)
        def _(t, group=group, qs=qs):
            slot = list_ref[t]
            row = lax.broadcasted_iota(jnp.int32, (BLK, BLK), 0)
            lane = lax.broadcasted_iota(jnp.int32, (1, BLK), 1)
            qid = sum((row >= cut_ref[i, d]).astype(jnp.int32) for d in range(ncut))
            kid = sum((lane >= cut_ref[slot, d]).astype(jnp.int32) for d in range(ncut))
            absorb(group, qs, [slot], qid == kid)

        outs = [acc_scr[k] / jnp.sum(l_scr[k], axis=1, keepdims=True) for k in range(len(group))]
        outs = [o.astype(jnp.bfloat16) for o in outs]
        if len(outs) % 2:
            outs.append(jnp.zeros_like(outs[0]))
        for k in range(0, len(outs), 2):
            tile = jnp.where(left, outs[k], outs[k + 1])
            lanes = slice((group[0] + k) // 2 * LANES, ((group[0] + k) // 2 + 1) * LANES)

            @pl.when(i < 2)
            def _(tile=tile, lanes=lanes):
                oa_ref[:, lanes] = tile

            @pl.when(i >= 2)
            def _(tile=tile, lanes=lanes):
                ob_ref[:, lanes] = tile


def attention(cuts, q, own, far, heads, head_dim):
    rows, width = q.shape
    scale = math.log2(math.e) * head_dim ** -0.5
    hbm = pl.BlockSpec(memory_space=pl.ANY)
    out = jax.ShapeDtypeStruct((rows // 2, width), jnp.bfloat16)
    scores = rows * 2 * rows * heads
    steps = -(-heads // GROUP)
    return pl.pallas_call(
        functools.partial(attention_kernel, scale=scale, heads=heads),
        out_shape=(out, out),
        grid_spec=pltpu.PrefetchScalarGridSpec(
            num_scalar_prefetch=1,
            grid=(rows // BLK,),
            in_specs=[pl.BlockSpec((BLK, width), lambda i, *_: (i, 0)), hbm, hbm],
            out_specs=(pl.BlockSpec((BLK, width), lambda i, *_: (jnp.minimum(i, 1), 0)), pl.BlockSpec((BLK, width), lambda i, *_: (jnp.maximum(i - 2, 0), 0))),
            scratch_shapes=[
                pltpu.VMEM((2 * rows, heads * LANES), jnp.bfloat16),
                pltpu.VMEM((GROUP, BLK, LANES), jnp.float32),
                pltpu.VMEM((GROUP, BLK, LANES), jnp.float32),
                pltpu.VMEM((GROUP, BLK, LANES), jnp.float32),
                pltpu.SMEM((16,), jnp.int32),
                pltpu.SemaphoreType.DMA((steps, 2)),
            ],
        ),
        compiler_params=pltpu.CompilerParams(dimension_semantics=("arbitrary",)),
        cost_estimate=pl.CostEstimate(flops=scores * 2 * LANES, bytes_accessed=(2 * rows * heads * LANES + 2 * rows * width) * 2, transcendentals=scores),
    )(cuts, q, own, far)


def solution(mesh):
    token_spec = P('dp', ('cp', 'sp'), None)
    seg_spec = P('dp', ('cp', 'sp'))
    axes = ('sp', 'cp')
    num = mesh.shape['cp'] * mesh.shape['sp']

    def core_of(f):
        return (f >> 1) & 1

    def stage1(f):
        return f ^ 1 if core_of(f) == 0 else f ^ 4

    def stage2(f):
        return f ^ 4 if core_of(f) == 0 else f ^ 1

    def spot(f):
        return (f & 1) * mesh.shape['cp'] + (f >> 1)

    perm_core = [(spot(f), spot(f ^ 2)) for f in range(num)]
    perm_one = [(spot(f), spot(stage1(f))) for f in range(num)]
    perm_cross = [(spot(f), spot(stage1(f ^ 2))) for f in range(num)]
    perm_two = [(spot(f), spot(stage2(f))) for f in range(num)]
    block_table = []
    for f in range(num):
        g = stage2(f)
        block_table.append([spot(b) for b in (f, f ^ 2, stage1(f), stage1(f) ^ 2, g, g ^ 2, stage1(g), stage1(g) ^ 2)])

    def local_layer(hidden, seg_ids, w_qkv, w_out):
        batch, tokens, dim = hidden.shape
        heads, head_dim = w_out.shape[0], w_out.shape[1]
        mine = heads // 2
        padded = -(-mine // GROUP) * GROUP
        per_core = batch // 2
        me = lax.axis_index('cp') * mesh.shape['sp'] + lax.axis_index('sp')
        core = (me // 2) % 2
        hsel = jnp.where(core == 0, me % 2, me // 4)

        def permute(x, perm):
            return lax.ppermute(x, axes, perm)

        xs = []
        turn = core
        for i in range(per_core):
            if i == 2:
                turn, xs[0] = lax.optimization_barrier((turn, xs[0]))
            keep = lax.dynamic_index_in_dim(hidden, turn * per_core + i, 0, keepdims=False)
            give = lax.dynamic_index_in_dim(hidden, (1 - turn) * per_core + i, 0, keepdims=False)
            xs.append([keep, permute(give, perm_core), permute(keep, perm_one), permute(give, perm_cross)])

        cuts = jnp.sum(seg_ids[:, :, None] < jnp.arange(1, 4), axis=1, dtype=jnp.int32)
        cuts = lax.all_gather(cuts, axes, axis=0)
        cuts = lax.dynamic_slice_in_dim(cuts, core * per_core, per_core, 1)
        pick = (jnp.asarray(block_table, jnp.int32)[me][:, None] == jnp.arange(num)).astype(jnp.int32)
        cuts = jnp.sum(pick[None, :, :, None] * jnp.transpose(cuts, (1, 0, 2))[:, None], axis=2)

        wt = jnp.transpose(w_qkv, (1, 2, 3, 0))
        sel = (hsel * mine).astype(jnp.int32).reshape(1)

        def out_weight(first):
            part = lax.dynamic_slice_in_dim(w_out, first * mine, mine, 0)
            return jnp.pad(part, ((0, padded - mine), (0, 0), (0, 0))).reshape(padded * head_dim, dim)

        wo_mine, wo_other = out_weight(hsel), out_weight(1 - hsel)

        qs, kvs, fars = [], [], []
        for i in range(per_core):
            q, kv = project_all(sel, xs[i], wt, mine, head_dim)
            sel, q = lax.optimization_barrier((sel, q))
            qs.append(q)
            kvs.append(kv)
            fars.append(permute(kv, perm_two))

        result = jnp.zeros((batch, tokens, dim), jnp.bfloat16)
        ys = []
        for i in range(per_core):
            cut = cuts[i]
            if i >= 2:
                cut, ys[i - 2] = lax.optimization_barrier((cut, ys[i - 2]))
            o_chip, o_next = attention(cut, qs[i], kvs[i], fars[i], mine, head_dim)
            cuts, o_chip = lax.optimization_barrier((cuts, o_chip))
            o_got = permute(o_next, perm_one)
            y = jnp.dot(o_chip, wo_mine, preferred_element_type=jnp.float32)
            y = (y + jnp.dot(o_got, wo_other, preferred_element_type=jnp.float32)).astype(jnp.bfloat16)
            ys.append(y)
        for i, y in enumerate(ys):
            y_got = permute(y[tokens:], perm_core)
            result = lax.dynamic_update_slice(result, y[None, :tokens], (core * per_core + i, 0, 0))
            result = lax.dynamic_update_slice(result, y_got[None], ((1 - core) * per_core + i, 0, 0))
        return result

    return jax.shard_map(local_layer, mesh=mesh, in_specs=(token_spec, seg_spec, P(), P()), out_specs=token_spec, check_vma=False)
```

```python
import functools
import math

import jax
import jax.numpy as jnp
from jax import lax
from jax.experimental import pallas as pl
from jax.experimental.pallas import tpu as pltpu
from jax.sharding import PartitionSpec as P


BLK = 256
LANES = 128
GROUP = 4
MASKED = -0.7 * 3.4028235e38
NT = (((1,), (1,)), ((), ()))


def project_kernel(sel_ref, x0, x1, x2, x3, w_ref, q_ref, kv_ref, x_scr, w_scr, x_sem, w_sem, *, heads, head_dim):
    g = pl.program_id(0)
    xs = (x0, x1, x2, x3)
    groups = [list(range(s, min(s + GROUP, heads))) for s in range(0, heads, GROUP)]
    kv_row = GROUP * head_dim

    def x_copies():
        return [pltpu.make_async_copy(x, x_scr.at[pl.ds(n * BLK, BLK), :], x_sem.at[n]) for n, x in enumerate(xs)]

    def w_copies(n):
        first = sel_ref[0]
        out = []
        for k, h in enumerate(groups[n]):
            swap = k % 2
            rows = [k + 1 - 2 * swap, kv_row // head_dim + 2 * k + 1 - swap, kv_row // head_dim + 2 * k + swap]
            for j, row in enumerate(rows):
                out.append(pltpu.make_async_copy(w_ref.at[j, first + h], w_scr.at[n, pl.ds(row * head_dim, head_dim), :], w_sem.at[n, 3 * k + j]))
        return out

    @pl.when(g == 0)
    def _():
        for c in x_copies():
            c.start()
        for c in w_copies(0):
            c.start()
        for n, group in enumerate(groups):
            for k in range(len(group), GROUP):
                swap = k % 2
                zero = jnp.zeros((head_dim, w_scr.shape[2]), w_scr.dtype)
                w_scr[n, (k + 1 - 2 * swap) * head_dim:(k + 2 - 2 * swap) * head_dim, :] = zero
                for r in range(2):
                    row = kv_row + (2 * k + r) * head_dim
                    w_scr[n, row:row + head_dim, :] = zero
        for c in x_copies():
            c.wait()

    for n in range(len(groups)):
        @pl.when(g == n)
        def _(n=n):
            for c in w_copies(n):
                c.wait()
            if n + 1 < len(groups):
                for c in w_copies(n + 1):
                    c.start()

    half = x_scr.shape[0] // 2
    for r in range(2):
        x = x_scr[r * half:(r + 1) * half, :]
        for n in range(w_scr.shape[1] // BLK):
            w = w_scr[g, n * BLK:(n + 1) * BLK, :]
            out = lax.dot_general(x, w, NT, preferred_element_type=jnp.float32).astype(jnp.bfloat16)
            if n == 0:
                q_ref[r * half:(r + 1) * half, :] = out
            else:
                kv_ref[r * half:(r + 1) * half, (n - 1) * BLK:n * BLK] = out


def project_all(sel, xs, wt, heads, head_dim):
    rows, dim = 4 * xs[0].shape[0], xs[0].shape[1]
    steps = pl.cdiv(heads, GROUP)
    wide = GROUP * head_dim
    out = (jax.ShapeDtypeStruct((rows, steps * wide), jnp.bfloat16), jax.ShapeDtypeStruct((rows, heads * 2 * head_dim), jnp.bfloat16))
    hbm = pl.BlockSpec(memory_space=pl.ANY)
    return pl.pallas_call(
        functools.partial(project_kernel, heads=heads, head_dim=head_dim),
        out_shape=out,
        grid_spec=pltpu.PrefetchScalarGridSpec(
            num_scalar_prefetch=1,
            grid=(steps,),
            in_specs=[hbm] * 5,
            out_specs=(pl.BlockSpec((rows, wide), lambda g, *_: (0, g)), pl.BlockSpec((rows, 2 * wide), lambda g, *_: (0, g))),
            scratch_shapes=[
                pltpu.VMEM((rows, dim), jnp.bfloat16),
                pltpu.VMEM((steps, 3 * wide, dim), jnp.bfloat16),
                pltpu.SemaphoreType.DMA((4,)),
                pltpu.SemaphoreType.DMA((steps, 3 * GROUP)),
            ],
        ),
        compiler_params=pltpu.CompilerParams(dimension_semantics=("arbitrary",)),
        cost_estimate=pl.CostEstimate(flops=2 * rows * dim * 3 * heads * head_dim, bytes_accessed=2 * (rows * dim * 3 + 3 * heads * head_dim * dim), transcendentals=0),
    )(sel, *xs, wt)


def attention_kernel(cut_ref, q_ref, own_ref, far_ref, oa_ref, ob_ref, kv_scr, m_scr, l_scr, acc_scr, list_ref, sem, *, scale, heads):
    i = pl.program_id(0)
    rows = own_ref.shape[0]
    blocks = 2 * rows // BLK
    ncut = cut_ref.shape[1]
    groups = [list(range(s, min(s + GROUP, heads))) for s in range(0, heads, GROUP)]
    left = lax.broadcasted_iota(jnp.int32, (BLK, LANES), 1) < LANES // 2

    def copies(n, size):
        cols = pl.ds(pl.multiple_of(n * GROUP * LANES, LANES), size * LANES)
        return [pltpu.make_async_copy(ref.at[:, cols], kv_scr.at[pl.ds(r * rows, rows), cols], sem.at[n, r]) for r, ref in enumerate((own_ref, far_ref))]

    @pl.when(i == 0)
    def _():
        for n, group in enumerate(groups):
            for c in copies(n, len(group)):
                c.start()

    def id_at(block, pos):
        return sum((cut_ref[block, d] <= pos).astype(jnp.int32) for d in range(ncut))

    qf, ql = id_at(i, 0), id_at(i, BLK - 1)
    count = jnp.int32(0)
    kinds = []
    for b in range(blocks):
        kf, kl = id_at(b, 0), id_at(b, BLK - 1)
        meets = ((kf <= ql) & (qf <= kl)).astype(jnp.int32)
        full = meets * ((qf == ql) & (kf == kl)).astype(jnp.int32)
        kinds.append(meets - full)
        list_ref[count] = b
        count = count + full
    quads = count // 4
    pairs_end = count // 2
    for b in range(blocks):
        list_ref[count] = b
        count = count + kinds[b]

    def lanes_at(tile):
        return pl.ds(pl.multiple_of(tile * LANES, LANES), LANES)

    def absorb(base, qs, slots, mask):
        starts = [pl.multiple_of(slot * BLK, BLK) for slot in slots]

        def kv_of(k):
            tiles = [kv_scr[pl.ds(s, BLK), lanes_at(base + k)] for s in starts]
            return tiles[0] if len(tiles) == 1 else jnp.concatenate(tiles, axis=0)

        def scores(k):
            s = lax.dot_general(qs[k], kv_of(k), NT, preferred_element_type=jnp.float32)
            return s if mask is None else jnp.where(mask, s, MASKED)

        ahead = scores(0)
        for k in range(len(qs)):
            s = ahead
            if k + 1 < len(qs):
                ahead = scores(k + 1)
            parts = [s[:, j * LANES:(j + 1) * LANES] for j in range(len(slots) * BLK // LANES)]
            mx = functools.reduce(jnp.maximum, parts)
            m_old = m_scr[k]
            m_new = jnp.maximum(m_old, jnp.max(mx, axis=1, keepdims=True))
            alpha = jnp.exp2((m_old - m_new) * scale)
            ps = [jnp.exp2((part - m_new) * scale) for part in parts]
            m_scr[k] = m_new
            l_scr[k] = l_scr[k] * alpha + functools.reduce(jnp.add, ps)
            p = jnp.concatenate([p.astype(jnp.bfloat16) for p in ps], axis=1)
            acc_scr[k] = acc_scr[k] * alpha + jnp.dot(p, kv_of(k), preferred_element_type=jnp.float32)

    def heads_of(n, size):
        base = n * GROUP

        @pl.when(i == 0)
        def _():
            for c in copies(n, size):
                c.wait()

        qs = []
        for k in range(size):
            tile = q_ref[:, lanes_at(base // 2 + k // 2)]
            zero = jnp.zeros_like(tile)
            qs.append(jnp.where(left, tile, zero) if k % 2 else jnp.where(left, zero, tile))
            m_scr[k] = jnp.full((BLK, LANES), MASKED, jnp.float32)
            l_scr[k] = jnp.zeros((BLK, LANES), jnp.float32)
            acc_scr[k] = jnp.zeros((BLK, LANES), jnp.float32)

        @pl.loop(0, quads)
        def _(t):
            absorb(base, qs, [list_ref[4 * t + u] for u in range(4)], None)

        @pl.loop(2 * quads, pairs_end)
        def _(t):
            absorb(base, qs, [list_ref[2 * t], list_ref[2 * t + 1]], None)

        @pl.loop(2 * pairs_end, count)
        def _(t):
            slot = list_ref[t]
            row = lax.broadcasted_iota(jnp.int32, (BLK, BLK), 0)
            lane = lax.broadcasted_iota(jnp.int32, (1, BLK), 1)
            qid = sum((row >= cut_ref[i, d]).astype(jnp.int32) for d in range(ncut))
            kid = sum((lane >= cut_ref[slot, d]).astype(jnp.int32) for d in range(ncut))
            absorb(base, qs, [slot], qid == kid)

        outs = [acc_scr[k] / jnp.sum(l_scr[k], axis=1, keepdims=True) for k in range(size)]
        outs = [o.astype(jnp.bfloat16) for o in outs]
        if len(outs) % 2:
            outs.append(jnp.zeros_like(outs[0]))
        for k in range(0, len(outs), 2):
            tile = jnp.where(left, outs[k], outs[k + 1])
            lanes = lanes_at(base // 2 + k // 2)

            @pl.when(i < 2)
            def _(tile=tile, lanes=lanes):
                oa_ref[:, lanes] = tile

            @pl.when(i >= 2)
            def _(tile=tile, lanes=lanes):
                ob_ref[:, lanes] = tile

    whole = [group for group in groups if len(group) == GROUP]

    @pl.loop(0, len(whole))
    def _(n):
        heads_of(n, GROUP)

    for n in range(len(whole), len(groups)):
        heads_of(n, len(groups[n]))


def attention(cuts, q, own, far, heads, head_dim):
    rows, width = q.shape
    scale = math.log2(math.e) * head_dim ** -0.5
    hbm = pl.BlockSpec(memory_space=pl.ANY)
    out = jax.ShapeDtypeStruct((rows // 2, width), jnp.bfloat16)
    scores = rows * 2 * rows * heads
    steps = -(-heads // GROUP)
    return pl.pallas_call(
        functools.partial(attention_kernel, scale=scale, heads=heads),
        out_shape=(out, out),
        grid_spec=pltpu.PrefetchScalarGridSpec(
            num_scalar_prefetch=1,
            grid=(rows // BLK,),
            in_specs=[pl.BlockSpec((BLK, width), lambda i, *_: (i, 0)), hbm, hbm],
            out_specs=(pl.BlockSpec((BLK, width), lambda i, *_: (jnp.minimum(i, 1), 0)), pl.BlockSpec((BLK, width), lambda i, *_: (jnp.maximum(i - 2, 0), 0))),
            scratch_shapes=[
                pltpu.VMEM((2 * rows, heads * LANES), jnp.bfloat16),
                pltpu.VMEM((GROUP, BLK, LANES), jnp.float32),
                pltpu.VMEM((GROUP, BLK, LANES), jnp.float32),
                pltpu.VMEM((GROUP, BLK, LANES), jnp.float32),
                pltpu.SMEM((16,), jnp.int32),
                pltpu.SemaphoreType.DMA((steps, 2)),
            ],
        ),
        compiler_params=pltpu.CompilerParams(dimension_semantics=("arbitrary",)),
        cost_estimate=pl.CostEstimate(flops=scores * 2 * LANES, bytes_accessed=(2 * rows * heads * LANES + 2 * rows * width) * 2, transcendentals=scores),
    )(cuts, q, own, far)


def out_kernel(chip_ref, got_ref, mine_ref, other_ref, keep_ref, give_ref):
    half = keep_ref.shape[0]
    y = jnp.dot(chip_ref[...], mine_ref[...], preferred_element_type=jnp.float32)
    y = (y + jnp.dot(got_ref[...], other_ref[...], preferred_element_type=jnp.float32)).astype(jnp.bfloat16)
    keep_ref[...] = y[:half]
    give_ref[...] = y[half:]


def project_out(o_chip, o_got, wo_mine, wo_other):
    rows, depth = o_chip.shape
    dim = wo_mine.shape[1]
    step = dim // 3
    o_spec = pl.BlockSpec((rows, depth), lambda n: (0, 0))
    w_spec = pl.BlockSpec((depth, step), lambda n: (0, n))
    out_spec = pl.BlockSpec((rows // 2, step), lambda n: (0, n))
    out = jax.ShapeDtypeStruct((rows // 2, dim), jnp.bfloat16)
    return pl.pallas_call(
        out_kernel,
        out_shape=(out, out),
        grid=(3,),
        in_specs=[o_spec, o_spec, w_spec, w_spec],
        out_specs=(out_spec, out_spec),
        compiler_params=pltpu.CompilerParams(dimension_semantics=("arbitrary",)),
        cost_estimate=pl.CostEstimate(flops=4 * rows * depth * dim, bytes_accessed=4 * (rows * depth + depth * dim) + 2 * rows * dim, transcendentals=0),
    )(o_chip, o_got, wo_mine, wo_other)


def solution(mesh):
    token_spec = P('dp', ('cp', 'sp'), None)
    seg_spec = P('dp', ('cp', 'sp'))
    axes = ('sp', 'cp')
    num = mesh.shape['cp'] * mesh.shape['sp']

    def core_of(f):
        return (f >> 1) & 1

    def stage1(f):
        return f ^ 1 if core_of(f) == 0 else f ^ 4

    def stage2(f):
        return f ^ 4 if core_of(f) == 0 else f ^ 1

    def spot(f):
        return (f & 1) * mesh.shape['cp'] + (f >> 1)

    perm_core = [(spot(f), spot(f ^ 2)) for f in range(num)]
    perm_one = [(spot(f), spot(stage1(f))) for f in range(num)]
    perm_cross = [(spot(f), spot(stage1(f ^ 2))) for f in range(num)]
    perm_two = [(spot(f), spot(stage2(f))) for f in range(num)]
    block_table = []
    for f in range(num):
        g = stage2(f)
        block_table.append([spot(b) for b in (f, f ^ 2, stage1(f), stage1(f) ^ 2, g, g ^ 2, stage1(g), stage1(g) ^ 2)])

    def local_layer(hidden, seg_ids, w_qkv, w_out):
        batch, tokens, dim = hidden.shape
        heads, head_dim = w_out.shape[0], w_out.shape[1]
        mine = heads // 2
        padded = -(-mine // GROUP) * GROUP
        per_core = batch // 2
        me = lax.axis_index('cp') * mesh.shape['sp'] + lax.axis_index('sp')
        core = (me // 2) % 2
        hsel = jnp.where(core == 0, me % 2, me // 4)

        def permute(x, perm):
            return lax.ppermute(x, axes, perm)

        def fetch(i, turn):
            keep = lax.dynamic_index_in_dim(hidden, turn * per_core + i, 0, keepdims=False)
            give = lax.dynamic_index_in_dim(hidden, (1 - turn) * per_core + i, 0, keepdims=False)
            out = [keep]
            for part, perm in ((give, perm_core), (keep, perm_one), (give, perm_cross)):
                out.append(permute(part, perm))
            return out

        wt = jnp.transpose(w_qkv, (1, 2, 3, 0))
        sel = (hsel * mine).astype(jnp.int32).reshape(1)

        def out_weight(first):
            part = lax.dynamic_slice_in_dim(w_out, first * mine, mine, 0)
            return jnp.pad(part, ((0, padded - mine), (0, 0), (0, 0))).reshape(padded * head_dim, dim)

        wo_mine, wo_other = out_weight(hsel), out_weight(1 - hsel)

        def gather_cuts(seg):
            cuts = jnp.sum(seg[:, :, None] < jnp.arange(1, 4), axis=1, dtype=jnp.int32)
            cuts = lax.all_gather(cuts, axes, axis=0)
            cuts = lax.dynamic_slice_in_dim(cuts, core * per_core, per_core, 1)
            pick = (jnp.asarray(block_table, jnp.int32)[me][:, None] == jnp.arange(num)).astype(jnp.int32)
            return jnp.sum(pick[None, :, :, None] * jnp.transpose(cuts, (1, 0, 2))[:, None], axis=2)

        order = (sel, core)
        xs = [fetch(0, core), fetch(1, core)]
        qs, kvs, fars, ys = [], [], [], []

        def project_next(order):
            q, kv = project_all(order[0], xs[len(qs)], wt, mine, head_dim)
            fars.append(permute(kv, perm_two))
            kvs.append(kv)
            order, q = lax.optimization_barrier((order, q))
            qs.append(q)
            return order

        order = project_next(order)
        order = project_next(order)
        order, seg = lax.optimization_barrier((order, seg_ids))
        xs.append(fetch(2, order[1]))
        order = order + (gather_cuts(seg),)
        for i in range(per_core):
            if i >= 2:
                order, ys[i - 2] = lax.optimization_barrier((order, ys[i - 2]))
            o_chip, o_next = attention(order[2][i], qs[i], kvs[i], fars[i], mine, head_dim)
            order, o_chip = lax.optimization_barrier((order, o_chip))
            o_got = permute(o_next, perm_one)
            if i + 2 < per_core:
                order = project_next(order)
            if i + 3 < per_core:
                xs.append(fetch(i + 3, order[1]))
            y = project_out(o_chip, o_got, wo_mine, wo_other)
            ys.append(y)
        result = jnp.zeros((batch, tokens, dim), jnp.bfloat16)
        for i, (keep, give) in enumerate(ys):
            got = permute(give, perm_core)
            result = lax.dynamic_update_slice(result, keep[None], (core * per_core + i, 0, 0))
            result = lax.dynamic_update_slice(result, got[None], ((1 - core) * per_core + i, 0, 0))
        return result


    return jax.shard_map(local_layer, mesh=mesh, in_specs=(token_spec, seg_spec, P(), P()), out_specs=token_spec, check_vma=False)
```
